512 devices in a mesh: dp: 64 (over z, y), tm: 8 (over x, core).
Axes of the slice: x: 4, y: 8, z: 8, core: 2. Of those that a mesh axis runs over, the one named last changes fastest.
Arguments:
- hidden: bfloat16 [128, 1024, 4096], P('dp', 'tm'), may hold values from -6 to 6
- first_weight: bfloat16 [4096, 1024], P('dp'), may hold values from -0.09375 to 0.09375
- first_bias: float32 [1024], replicated, may hold values from -3 to 3
- second_weight: float32 [1024], replicated, may hold values from -0.1875 to 0.1875
- second_bias: float32 [1], replicated, may hold values from -3 to 3
- rewards: float32 [128, 1024], P('dp', 'tm'), may hold values from -0.8 to 0.8
- dones: int32 [128, 1024], P('dp', 'tm'), may hold values 0 or 1
- lengths: int32 [128], P('dp'), may hold values from 512 to 1024
- discount: float32 [128], P('dp'), may hold values from 0.96 to 1
- trace: float32 [128], P('dp'), may hold values from 0.99902344 to 1
Outputs:
- advantages: float32 [128, 1024], P('dp', 'tm')
- returns: float32 [128, 1024], P('dp', 'tm')
The draws below stay inside these ranges and needn't reach their ends.
All inputs are finite; a program needn't handle non-finite values. No bound on the sum of `dones` on one device may be relied on, other than what follows from the above.
Results may differ from the reference program's by a relative error of at most 0.0003.
Values may be sent and summed in bfloat16 or wider, within the bound.
A program may use at most 64 MiB of HBM per device.

```python
import jax
import jax.numpy as jnp
from jax import lax

D = 4096
CRITIC = 1024
TRAJ = 128
STEPS = 1024


def draw_discount(key, part):
    uniform_draw = jax.random.uniform(jax.random.fold_in(key, 11), (TRAJ,), jnp.float32)
    low_rate = jnp.log(0.3)
    high_rate = jnp.log(STEPS / 25.0)
    rate = jnp.exp(low_rate + uniform_draw * (high_rate - low_rate))
    return jnp.exp(-rate / STEPS).astype(jnp.float32)


def draw_trace(key, part):
    uniform_draw = jax.random.uniform(jax.random.fold_in(key, 23), (TRAJ,), jnp.float32)
    rate = jnp.exp(jnp.log(0.1) + uniform_draw * (jnp.log(1.0) - jnp.log(0.1)))
    return jnp.exp(-rate / STEPS).astype(jnp.float32)


def touch_ends(array, rng, low, largest):
    longest = array.shape.index(max(array.shape))
    spots = []
    for shift in (0, 1):
        where = [jax.random.randint(jax.random.fold_in(rng, axis), (), 0, length) for axis, length in enumerate(array.shape)]
        where[longest] = (where[longest] + shift) % array.shape[longest]
        spots.append(tuple(where))
    return array.at[spots[0]].set(low).at[spots[1]].set(largest)


def block_levels(stream_key, extent, split, least, top_value):
    factor_of, own = 1.0, jax.random.fold_in(stream_key, 6)
    for axis_at, shards_of in split:
        heights = jnp.exp(jax.random.uniform(jax.random.fold_in(own, axis_at), (shards_of,), jnp.float32, least / len(split), top_value / len(split)))
        factor_of = factor_of * jnp.repeat(heights, extent[axis_at] // shards_of).reshape([-1 if axis == axis_at else 1 for axis in range(len(extent))])
    return factor_of


def noise(key, dims, deviation, limit, split=(), kind=jnp.bfloat16):
    level = block_levels(key, dims, split, -0.22, 0.18) if split else 1.0
    entries = jax.random.normal(key, dims, jnp.float32) * deviation * level
    return jnp.minimum(jnp.maximum(entries, -limit), limit).astype(kind)


def setup_inputs(seed: int = 0) -> dict:
    splits = jax.random.split(jax.random.key(seed), 11)
    return {
        "hidden": noise(splits[0], (TRAJ, STEPS, D), 1.0, 6.0, ((0, 64), (1, 8))),
        "first_weight": noise(splits[1], (D, CRITIC), D ** -0.5, 0.09375, ((0, 64),)),
        "first_bias": noise(splits[2], (CRITIC,), 0.5, 3.0, (), jnp.float32),
        "second_weight": noise(splits[3], (CRITIC,), CRITIC ** -0.5, 0.1875, (), jnp.float32),
        "second_bias": noise(splits[4], (1,), 1.0, 3.0, (), jnp.float32),
        "rewards": noise(splits[5], (TRAJ, STEPS), 0.1, 0.8, ((0, 64), (1, 8)), jnp.float32),
        "dones": touch_ends((jax.random.randint(splits[6], (TRAJ, STEPS), 0, 256) < 1).astype(jnp.int32), jax.random.fold_in(splits[6], 1), 0, 1),
        "lengths": touch_ends(jax.random.randint(splits[7], (TRAJ,), STEPS // 2, STEPS + 1), jax.random.fold_in(splits[7], 1), STEPS // 2, STEPS).astype(jnp.int32),
        "discount": draw_discount(jax.random.fold_in(splits[10], 71), 0),
        "trace": draw_trace(jax.random.fold_in(splits[10], 71), 0),
    }


def reference(hidden, first_weight, first_bias, second_weight, second_bias, rewards, dones, lengths, discount, trace):

    def critic_one(trajectory):
        pre = jnp.dot(trajectory, first_weight, preferred_element_type=jnp.float32)
        return jnp.dot(jax.nn.silu(pre + first_bias), second_weight, precision=lax.Precision.HIGHEST) + second_bias[0]
    values = lax.map(critic_one, hidden)
    time_index = jnp.arange(STEPS, dtype=jnp.int32)
    live = (time_index[None, :] < lengths[:, None]).astype(jnp.float32)
    live_next = ((time_index + 1)[None, :] < lengths[:, None]).astype(jnp.float32)
    keep = 1.0 - dones.astype(jnp.float32)
    value_next = jnp.concatenate([values[:, 1:], jnp.zeros((values.shape[0], 1), jnp.float32)], axis=1)
    gamma = discount[:, None]
    delta = live * (rewards + gamma * keep * live_next * value_next - values)
    decay = gamma * trace[:, None] * keep * live_next

    def backward(running, inputs):
        updated = inputs[1] + inputs[0] * running
        return (updated, updated)
    start = jnp.zeros((values.shape[0],), jnp.float32)
    _, gains = lax.scan(backward, start, (decay.T, delta.T), reverse=True)
    gain = gains.T
    returns = live * (gain + values)
    count = jnp.sum(live)
    mean = jnp.sum(gain) / count
    spread = jnp.sum(live * (gain - mean) ** 2) / count
    advantages = live * (gain - mean) / jnp.sqrt(spread + 1e-06)
    return (advantages, returns)
```

```python
import functools

import jax
import jax.numpy as jnp
from jax import lax
from jax.experimental import pallas as pl
from jax.experimental.pallas import tpu as pltpu
from jax.sharding import Mesh
from jax.sharding import PartitionSpec as P

MESH = pl.DeviceIdType.MESH
DP = ("z", "y")
TM = ("x", "c")


def offsets(n):
    return list(range(-(n // 2 - 1), n // 2 + 1))


def kernel(
    sizes,
    hid, w, b1, w2, rew, don, ln, gm, tr, b2,
    adv, ret,
    H, WA, WB, acc, V, RK, PK, C, GN, G,
    h_loc, w_loc, h_send, h_recv, a_recv, b_recv, w_send,
    rk_send, rk_recv, v_send, v_recv, g_send, g_recv,
):
    NZ, NY, NX = sizes
    NB = NX * 2
    z, y, x, c = (lax.axis_index(a) for a in ("z", "y", "x", "c"))
    (traj, steps), depth = rew.shape, w.shape[0]
    rows = traj * steps
    half = WA.shape[-1]

    def wrap(v, n):
        return lax.rem(v + n, n)

    def remote(src, dst, ss, rs, dev):
        return pltpu.make_async_remote_copy(
            src_ref=src, dst_ref=dst, send_sem=ss, recv_sem=rs, device_id=dev, device_id_type=MESH
        )

    tm_peers = [(i, j) for i in range(NX) for j in range(2) if (i, j) != (0, 0)]
    dp_peers = [(i, j) for i in range(NZ) for j in range(NY) if (i, j) != (0, 0)]

    loads = []
    for p, W in enumerate((WA, WB)):
        cols = pl.ds(pl.multiple_of(c * 2 * half + p * half, half), half)
        loads.append(pltpu.make_async_copy(w.at[:, cols], W.at[z, pl.ds(pl.multiple_of(y * depth, depth), depth)], w_loc.at[p]))
    own_h = H.at[pl.ds(pl.multiple_of(c * rows, rows), rows)]
    loads.append(pltpu.make_async_copy(hid, own_h, h_loc))
    for copy in loads:
        copy.start()

    keep = 1.0 - don[...].astype(jnp.float32)
    RK[x, c, 0:2] = rew[...]
    RK[x, c, 2:4] = keep

    barrier = pltpu.get_barrier_semaphore()
    near = [{"z": wrap(z + 1, NZ)}, {"z": wrap(z - 1, NZ)}, {"y": wrap(y + 1, NY)}, {"y": wrap(y - 1, NY)}]
    far = [{"x": wrap(x + i, NX), "c": wrap(c + j, 2)} for i, j in tm_peers]
    for dev in near + far:
        pl.semaphore_signal(barrier, inc=1, device_id=dev, device_id_type=MESH)
    pl.semaphore_wait(barrier, len(near) + len(far))
    loads[0].wait()
    loads[1].wait()

    oz, oy = offsets(NZ), offsets(NY)
    sends = []
    n_oz, n_oy = len(oz), len(oy)
    sem_of = {(ry, rz): (ry - oy[0]) * n_oz + (rz - oz[0]) for ry in oy for rz in oz}
    zabs = {rz: wrap(z + rz, NZ) for rz in oz}
    yabs = {ry: wrap(y + ry, NY) for ry in oy}

    def place(W, ry, rz):
        return W.at[zabs[rz], pl.ds(pl.multiple_of(yabs[ry] * depth, depth), depth)]

    def hop(part, piece, axis, way):
        ry, rz = piece
        W, sem = (WA, a_recv) if part == 0 else (WB, b_recv)
        n, o = (NZ, rz) if axis == "z" else (NY, ry)
        new = o - way
        if new == -(n // 2):
            new = n // 2
        there = (ry, new) if axis == "z" else (new, rz)
        here = z if axis == "z" else y
        k = len(sends)
        copy = remote(place(W, ry, rz), place(W, ry, rz), w_send.at[k], sem.at[sem_of[there]], {axis: wrap(here + way, n)})
        copy.start()
        sends.append(copy)

    def forwards(part, piece):
        ry, rz = piece
        (ax1, n1, o1), (ax2, n2, o2) = (("z", NZ, rz), ("y", NY, ry)) if part == 0 else (("y", NY, ry), ("z", NZ, rz))
        out = []

        def ahead(n, o, way, last_ok):
            d = abs(o) + 1
            return d < n // 2 or (d == n // 2 and last_ok)

        if o2 == 0:
            for way in (1, -1):
                if o1 == 0 or (o1 < 0) == (way > 0) and abs(o1) < n1 // 2:
                    if ahead(n1, o1, way, way == 1):
                        out.append((ax1, way))
        for way in (1, -1):
            if o2 == 0 or ((o2 < 0) == (way > 0) and abs(o2) < n2 // 2):
                ok = (o1 % 2 == 0) == (way == 1)
                if ahead(n2, o2, way, ok):
                    out.append((ax2, way))
        return out

    for part in (0, 1):
        for axis, way in forwards(part, (0, 0)):
            hop(part, (0, 0), axis, way)

    mate = {"c": 1 - c}
    h_copy = remote(hid, own_h, h_send, h_recv, mate)
    h_copy.start()
    rk_copies = []
    for k, (i, j) in enumerate(tm_peers):
        copy = remote(RK.at[x, c], RK.at[x, c], rk_send.at[k], rk_recv.at[k], far[k])
        copy.start()
        rk_copies.append(copy)

    def tables():
        for copy in rk_copies:
            copy.wait_recv()
        rew16 = jnp.concatenate([RK[b // 2, b % 2, 0:2] for b in range(NB)], axis=0)
        keep16 = jnp.concatenate([RK[b // 2, b % 2, 2:4] for b in range(NB)], axis=0)
        row = lax.broadcasted_iota(jnp.int32, rew16.shape, 0)
        lane = lax.broadcasted_iota(jnp.int32, rew16.shape, 1)
        t = (row // 2) * steps + lane
        odd = row % 2 == 1
        length = jnp.where(odd, ln[1], ln[0])
        gamma = jnp.where(odd, gm[1], gm[0])
        lam = jnp.where(odd, tr[1], tr[0])
        live = (t < length).astype(jnp.float32)
        live_next = (t + 1 < length).astype(jnp.float32)
        C[0] = live
        C[1] = live * rew16
        C[2] = live * gamma * keep16 * live_next
        prod = gamma * lam * keep16 * live_next
        k, span = 0, 1
        while span < NB * steps:
            PK[k] = prod
            prod = prod * shifted(prod, span)
            k, span = k + 1, span * 2

    def shifted(v, span):
        n = NB * 2
        if span >= steps:
            r = 2 * (span // steps)
            return jnp.concatenate([v[r:], v[:r]], axis=0)
        rolled = pltpu.roll(v, steps - span, 1)
        lane = lax.broadcasted_iota(jnp.int32, v.shape, 1)
        return jnp.where(lane < steps - span, rolled, jnp.concatenate([rolled[2:], rolled[:2]], axis=0))

    def matmul(rz, first):
        zz = zabs[rz]
        k = NY * depth
        ks = pl.ds(pl.multiple_of(zz * k, k), k)
        for p, W in enumerate((WA, WB)):
            wv = W[zz]
            for r in range(2):
                rs = pl.ds(r * rows, rows)
                d = jnp.dot(H[rs, ks], wv, preferred_element_type=jnp.float32)
                if first:
                    acc[p, rs] = d
                else:
                    acc[p, rs] += d

    levels = {}
    for ry in oy:
        for rz in oz:
            if (ry, rz) != (0, 0):
                levels.setdefault(abs(ry) + abs(rz), []).append((ry, rz))
    last = max(levels)
    started = False
    for level in range(1, last + 1):
        todo = []
        for ry, rz in levels[level]:
            for part in (0, 1):
                second = ry if part == 0 else rz
                todo.append((abs(second), part, (ry, rz)))
        todo.sort(key=lambda e: (e[0], e[2], e[1]))
        for _, part, piece in todo:
            W, sem = (WA, a_recv) if part == 0 else (WB, b_recv)
            spot = place(W, *piece)
            pltpu.make_async_copy(spot, spot, sem.at[sem_of[piece]]).wait()
            for axis, way in forwards(part, piece):
                hop(part, piece, axis, way)
        if level == 1:
            tables()
        for rz in oz:
            if abs(rz) + NY // 2 == level:
                if not started:
                    loads[2].wait()
                    h_copy.wait_recv()
                matmul(rz, not started)
                started = True

    for r in range(2 * traj):
        rs = pl.ds(r * steps, steps)
        total = jnp.zeros((steps, 128), jnp.float32)
        for p in range(2):
            for q in range(half // 128):
                u = c * (2 * half // 128) + p * (half // 128) + q
                v = acc[p, rs, q * 128:(q + 1) * 128] + b1[pl.ds(u, 1), :]
                total += v / (1.0 + jnp.exp(-v)) * w2[pl.ds(u, 1), :]
        V[c, x, r:r + 1] = jnp.sum(total.T, axis=0, keepdims=True)

    v_copies = []
    for k, (i, j) in enumerate(tm_peers):
        copy = remote(V.at[c, x], V.at[c, x], v_send.at[k], v_recv.at[k], far[k])
        copy.start()
        v_copies.append(copy)
    for copy in sends:
        copy.wait_send()
    h_copy.wait_send()
    for copy in rk_copies:
        copy.wait_send()
    for copy in v_copies:
        copy.wait_recv()

    both = V[0] + V[1]
    v16 = jnp.concatenate([both[b // 2, 2 * (b % 2):2 * (b % 2) + 2] for b in range(NB)], axis=0) + b2[0]
    live = C[0]
    gain = C[1] - live * v16 + C[2] * shifted(v16, 1)
    k, span = 0, 1
    while span < NB * steps:
        gain = gain + PK[k] * shifted(gain, span)
        k, span = k + 1, span * 2

    G[z, y, 0:1] = jnp.sum(gain, axis=0, keepdims=True)
    G[z, y, 1:2] = jnp.sum(gain * gain, axis=0, keepdims=True)
    G[z, y, 2:3] = jnp.sum(live, axis=0, keepdims=True)
    G[z, y, 3:4] = jnp.zeros((1, steps), jnp.float32)
    g_copies = []
    for k, (i, j) in enumerate(dp_peers):
        copy = remote(G.at[z, y], G.at[z, y], g_send.at[k], g_recv.at[k], {"z": wrap(z + i, NZ), "y": wrap(y + j, NY)})
        copy.start()
        g_copies.append(copy)

    back = live * (gain + v16)
    for b in range(NB):
        GN[0, b] = gain[2 * b:2 * b + 2]
        GN[1, b] = back[2 * b:2 * b + 2]
        GN[2, b] = live[2 * b:2 * b + 2]
    me = x * 2 + c
    ret[...] = GN[1, me]
    for copy in v_copies + g_copies:
        copy.wait_send()
    for copy in g_copies:
        copy.wait_recv()
    sums = jnp.sum(jnp.sum(G[...], axis=(0, 1)), axis=1, keepdims=True)
    count = sums[2:3]
    mean = sums[0:1] / count
    spread = sums[1:2] / count - mean * mean
    adv[...] = GN[2, me] * (GN[0, me] - mean) / jnp.sqrt(spread + 1e-06)


def on_device(sizes, hidden, first_weight, first_bias, second_weight, second_bias, rewards, dones, lengths, discount, trace):
    NZ, NY, NX = sizes
    traj, steps, feats = hidden.shape
    depth, units = first_weight.shape
    half = units // 4
    rows = traj * steps
    NB = NX * 2
    vmem = pl.BlockSpec(memory_space=pltpu.VMEM)
    smem = pl.BlockSpec(memory_space=pltpu.SMEM)
    hbm = pl.BlockSpec(memory_space=pl.ANY)
    shape = jax.ShapeDtypeStruct(rewards.shape, jnp.float32)
    dma = pltpu.SemaphoreType.DMA
    n_pieces = NZ * NY
    return pl.pallas_call(
        functools.partial(kernel, sizes),
        out_shape=(shape, shape),
        in_specs=[hbm, hbm, vmem, vmem, vmem, vmem, smem, smem, smem, smem],
        out_specs=(vmem, vmem),
        scratch_shapes=[
            pltpu.VMEM((2 * rows, feats), jnp.bfloat16),
            pltpu.VMEM((NZ, NY * depth, half), jnp.bfloat16),
            pltpu.VMEM((NZ, NY * depth, half), jnp.bfloat16),
            pltpu.VMEM((2, 2 * rows, half), jnp.float32),
            pltpu.VMEM((2, NX, 2 * traj, steps), jnp.float32),
            pltpu.VMEM((NX, 2, 4, steps), jnp.float32),
            pltpu.VMEM((10, 2 * NB, steps), jnp.float32),
            pltpu.VMEM((3, 2 * NB, steps), jnp.float32),
            pltpu.VMEM((3, NB, 2, steps), jnp.float32),
            pltpu.VMEM((NZ, NY, 4, steps), jnp.float32),
            dma, dma((2,)), dma, dma,
            dma((n_pieces,)), dma((n_pieces,)), dma((2 * n_pieces,)),
            dma((NB - 1,)), dma((NB - 1,)), dma((NB - 1,)), dma((NB - 1,)),
            dma((n_pieces - 1,)), dma((n_pieces - 1,)),
        ],
        compiler_params=pltpu.CompilerParams(collective_id=0, has_side_effects=True, vmem_limit_bytes=60 << 20),
    )(
        hidden.reshape(rows, feats), first_weight, first_bias.reshape(-1, 128), second_weight.reshape(-1, 128),
        rewards, dones, lengths, discount, trace, second_bias,
    )


def solution(mesh):
    split = Mesh(mesh.devices.reshape(8, 8, 4, 2), ("z", "y", "x", "c"))
    placed = (
        P(DP, TM, None), P(DP, None), P(), P(), P(), P(DP, TM), P(DP, TM), P(DP), P(DP), P(DP),
    )
    return jax.shard_map(
        functools.partial(on_device, (8, 8, 4)),
        mesh=split, in_specs=placed, out_specs=(P(DP, TM), P(DP, TM)), check_vma=False,
    )
```

```python
import functools

import jax
import jax.numpy as jnp
from jax import lax
from jax.experimental import pallas as pl
from jax.experimental.pallas import tpu as pltpu
from jax.sharding import Mesh
from jax.sharding import PartitionSpec as P

MESH = pl.DeviceIdType.MESH
CHAIN = ((1,), (1,), (1,), (1,))
SKIP = ((1,), (1, 2), (2,), ())
SKIP2 = ((1,), (1,), (1, 2), ())
PAIRS = ((1, 2), (), (1, 2), ())
TABLES_AT = 60
ACROSS_AFTER = 14
HELD = 1
DP = ("z", "y")
TM = ("x", "c")


def offsets(n):
    return list(range(-(n // 2 - 1), n // 2 + 1))


def kernel(
    sizes,
    hid, w, b1, w2, rew, don, ln, gm, tr, b2,
    out,
    H, A, B, X, acc, V, RK, PK, C, GN, G, rewv, donv, b1v, w2v, lns, gms, trs, b2s,
    ld, h_send, h_recv, a_recv, b_recv, w_send, x_send, x_recv,
    rk_send, rk_recv, v_send, v_recv, g_send, g_recv,
):
    NZ, NY, NX = sizes
    NB = NX * 2
    z, y, x, c = (lax.axis_index(a) for a in ("z", "y", "x", "c"))
    (traj, steps), depth = rew.shape, w.shape[0]
    rows = traj * steps
    par = lax.rem(x, 2)
    q, e = depth // 4, depth // 2

    def wrap(v, n):
        return lax.rem(v + n, n)

    def remote(src, dst, ss, rs, dev):
        return pltpu.make_async_remote_copy(
            src_ref=src, dst_ref=dst, send_sem=ss, recv_sem=rs, device_id=dev, device_id_type=MESH
        )

    tm_peers = [(i, j) for i in range(NX) for j in range(2) if (i, j) != (0, 0)]
    dp_peers = [(i, j) for i in range(NZ) for j in range(NY) if (i, j) != (0, 0)]

    loads = []

    def load(src, dst):
        copy = pltpu.make_async_copy(src, dst, ld.at[len(loads)])
        copy.start()
        loads.append(copy)

    def block(j):
        return pl.ds(pl.multiple_of((c * 4 + j) * 128, 128), 128)

    load(rew, rewv)
    load(don, donv)
    own, other = 1 + 2 * par, 3 - 2 * par
    for p, W in enumerate((A, B)):
        load(w.at[p * e:(p + 1) * e, block(0)], W.at[z, y, 0:e])
        load(w.at[p * e:(p + 1) * e, block(own)], W.at[z, y, e:2 * e])
        load(w.at[pl.ds(pl.multiple_of(par * e + p * q, q), q), block(2)], W.at[z, y, 2 * e:2 * e + q])
    n_weights = len(loads)
    own_h = H.at[pl.ds(pl.multiple_of(c * rows, rows), rows)]
    load(hid, own_h)
    for src, dst in ((b1, b1v), (w2, w2v), (ln, lns), (gm, gms), (tr, trs), (b2, b2s)):
        load(src, dst)

    for copy in loads[:2]:
        copy.wait()
    RK[x, c, 0:2] = rewv[...]
    RK[x, c, 2:4] = 1.0 - donv[...].astype(jnp.float32)

    barrier = pltpu.get_barrier_semaphore()
    near = [{"z": wrap(z + d, NZ)} for d in (1, -1, 2, -2)] + [{"y": wrap(y + d, NY)} for d in (1, -1, 2, -2)]
    far = [{"x": wrap(x + i, NX), "c": wrap(c + j, 2)} for i, j in tm_peers]
    for dev in near + far:
        pl.semaphore_signal(barrier, inc=1, device_id=dev, device_id_type=MESH)
    pl.semaphore_wait(barrier, len(near) + len(far))
    for copy in loads[2:n_weights]:
        copy.wait()

    oz, oy = offsets(NZ), offsets(NY)
    sends = []
    n_oz = len(oz)
    sem_of = {(ry, rz): (ry - oy[0]) * n_oz + (rz - oz[0]) for ry in oy for rz in oz}
    zabs = {rz: wrap(z + rz, NZ) for rz in oz}
    yabs = {ry: wrap(y + ry, NY) for ry in oy}

    def place(part, piece):
        ry, rz = piece
        return (A, B)[part].at[zabs[rz], yabs[ry]]

    def norm(o, n):
        return o + n if o < -(n // 2 - 1) else o

    def hop(part, piece, axis, by):
        ry, rz = piece
        sem = (a_recv, b_recv)[part]
        there = (ry, norm(rz - by, NZ)) if axis == "z" else (norm(ry - by, NY), rz)
        here, n = (z, NZ) if axis == "z" else (y, NY)
        spot = place(part, piece)
        copy = remote(spot, spot, w_send.at[len(sends)], sem.at[sem_of[there]], {axis: wrap(here + by, n)})
        copy.start()
        sends.append(copy)

    def across(part, piece):
        ry, rz = piece
        src = place(part, piece).at[e:2 * e + q]
        dst = X.at[zabs[rz], yabs[ry], part * (e + q):(part + 1) * (e + q)]
        by = 1 - 2 * part
        remote(src, dst, x_send, x_recv.at[rz - oz[0]], {"x": wrap(x + by, NX)}).start()

    def forwards(part, piece):
        ry, rz = piece
        (ax1, n1, o1), (ax2, n2, o2) = (("z", NZ, rz), ("y", NY, ry)) if part == 0 else (("y", NY, ry), ("z", NZ, rz))
        first, second = [], []

        def onward(tree, n, o, last):
            out = []
            for way in (1, -1):
                if o == 0 or ((o < 0) == (way > 0) and abs(o) < n // 2):
                    for j in tree[abs(o)]:
                        d = abs(o) + j
                        if d < n // 2 or (d == n // 2 and way == last):
                            out.append(way * j)
            return out

        if o2 == 0:
            first = [(ax1, by) for by in onward(PAIRS, n1, o1, 1)]
        tree = SKIP if abs(o1) >= 3 else CHAIN
        second = [(ax2, by) for by in onward(tree, n2, o2, 1 if o1 % 2 == 0 else -1)]
        return first + second

    for part in (0, 1):
        for axis, by in forwards(part, (0, 0)):
            hop(part, (0, 0), axis, by)
        across(part, (0, 0))

    mate = {"c": 1 - c}
    h_copy = remote(hid, own_h, h_send, h_recv, mate)
    h_copy.start()
    rk_copies = []
    for k, (i, j) in enumerate(tm_peers):
        copy = remote(RK.at[x, c], RK.at[x, c], rk_send.at[k], rk_recv.at[k], far[k])
        copy.start()
        rk_copies.append(copy)

    def tables():
        for copy in rk_copies:
            copy.wait_recv()
        for copy in loads[n_weights + 1:]:
            copy.wait()
        rew16 = jnp.concatenate([RK[b // 2, b % 2, 0:2] for b in range(NB)], axis=0)
        keep16 = jnp.concatenate([RK[b // 2, b % 2, 2:4] for b in range(NB)], axis=0)
        row = lax.broadcasted_iota(jnp.int32, rew16.shape, 0)
        lane = lax.broadcasted_iota(jnp.int32, rew16.shape, 1)
        t = (row // 2) * steps + lane
        odd = row % 2 == 1
        length = jnp.where(odd, lns[1], lns[0])
        gamma = jnp.where(odd, gms[1], gms[0])
        lam = jnp.where(odd, trs[1], trs[0])
        live = (t < length).astype(jnp.float32)
        live_next = (t + 1 < length).astype(jnp.float32)
        C[0] = live
        C[1] = live * rew16
        C[2] = live * gamma * keep16 * live_next
        prod = gamma * lam * keep16 * live_next
        k, span = 0, 1
        while span < NB * steps:
            PK[k] = prod
            prod = prod * shifted(prod, span)
            k, span = k + 1, span * 2

    def shifted(v, span):
        n = NB * 2
        if span >= steps:
            r = 2 * (span // steps)
            return jnp.concatenate([v[r:], v[:r]], axis=0)
        rolled = pltpu.roll(v, steps - span, 1)
        lane = lax.broadcasted_iota(jnp.int32, v.shape, 1)
        return jnp.where(lane < steps - span, rolled, jnp.concatenate([rolled[2:], rolled[:2]], axis=0))

    def hidden_rows(rz, r):
        k = NY * depth
        return H[pl.ds(r * rows, rows), pl.ds(pl.multiple_of(zabs[rz] * k, k), k)]

    def multiply(p, rz, blocks, first):
        wv = jnp.concatenate([jnp.concatenate(b, axis=0) for b in blocks], axis=1)
        for r in range(2):
            rs = pl.ds(r * rows, rows)
            d = jnp.dot(hidden_rows(rz, r), wv, preferred_element_type=jnp.float32)
            if first:
                acc[p, rs] = d
            else:
                acc[p, rs] += d

    def own_part(rz, first):
        zz = zabs[rz]
        block0 = [W[zz, j, 0:e] for j in range(NY) for W in (A, B)]
        mine = [W[zz, j, e:2 * e] for j in range(NY) for W in (A, B)]
        multiply(0, rz, (block0, mine), first)

    def across_part(rz, first):
        zz = zabs[rz]
        pltpu.make_async_copy(X.at[zz], X.at[zz], x_recv.at[rz - oz[0]]).wait()
        theirs, block2 = [], []
        for j in range(NY):
            theirs += [X[zz, j, 0:e], X[zz, j, e + q:2 * e + q]]
            a = jnp.concatenate([A[zz, j, 2 * e:], B[zz, j, 2 * e:]], axis=0)
            b = jnp.concatenate([X[zz, j, e:e + q], X[zz, j, 2 * e + q:]], axis=0)
            block2 += [jnp.where(par == 0, a, b), jnp.where(par == 0, b, a)]
        multiply(1, rz, (theirs, block2), first)

    def passed(part, piece):
        for axis, by in forwards(part, piece):
            hop(part, piece, axis, by)
        across(part, piece)

    def delay(tree, o):
        best = {0: 0.0}
        for d in range(abs(o)):
            for j in tree[d] if d in best else ():
                best[d + j] = best[d] + 1.9 + 0.5 * j
        return best[abs(o)]

    def arrival(part, piece):
        o1, o2 = (piece[1], piece[0]) if part == 0 else piece
        return delay(PAIRS, o1) + delay(SKIP if abs(o1) >= 3 else CHAIN, o2) + 0.1 * abs(o2)

    pieces = [(p, (ry, rz)) for p in (0, 1) for ry in oy for rz in oz if (ry, rz) != (0, 0)]
    pieces.sort(key=lambda e: (arrival(*e), e[1], e[0]))
    events = [(i, 0, p, piece) for i, (p, piece) in enumerate(pieces)]
    for rz in oz:
        done = max(i for i, _, _, piece in events if type(piece) is tuple and piece[1] == rz)
        events.append((done, 1, 0, rz))
        events.append((done + ACROSS_AFTER, 2, 0, rz))
    events.append((TABLES_AT, 3, 0, 0))
    firsts = {1: True, 2: True}
    held = []
    for t, kind, part, what in sorted(events, key=lambda ev: ev[:2]):
        if kind == 0:
            spot = place(part, what)
            pltpu.make_async_copy(spot, spot, (a_recv, b_recv)[part].at[sem_of[what]]).wait()
            if t < HELD:
                held.append((part, what))
                if t == HELD - 1:
                    for one in held:
                        passed(*one)
            else:
                passed(part, what)
        elif kind == 3:
            tables()
        else:
            if kind == 1 and firsts[1]:
                loads[n_weights].wait()
                h_copy.wait_recv()
            (own_part if kind == 1 else across_part)(what, firsts[kind])
            firsts[kind] = False

    for r in range(2 * traj):
        rs = pl.ds(r * steps, steps)
        total = jnp.zeros((steps, 128), jnp.float32)
        for p in range(2):
            for j, u in enumerate(((0, own), (other, 2))[p]):
                u = c * 4 + u
                v = acc[p, rs, j * 128:(j + 1) * 128] + b1v[pl.ds(u, 1), :]
                total += v / (1.0 + jnp.exp(-v)) * w2v[pl.ds(u, 1), :]
        V[c, x, r:r + 1] = jnp.sum(total.T, axis=0, keepdims=True)

    v_copies = []
    for k, (i, j) in enumerate(tm_peers):
        copy = remote(V.at[c, x], V.at[c, x], v_send.at[k], v_recv.at[k], far[k])
        copy.start()
        v_copies.append(copy)
    for copy in sends:
        copy.wait_send()
    pltpu.make_async_copy(X, X, x_send).wait()
    h_copy.wait_send()
    for copy in rk_copies:
        copy.wait_send()
    for copy in v_copies:
        copy.wait_recv()

    both = V[0] + V[1]
    v16 = jnp.concatenate([both[b // 2, 2 * (b % 2):2 * (b % 2) + 2] for b in range(NB)], axis=0) + b2s[0]
    live = C[0]
    gain = C[1] - live * v16 + C[2] * shifted(v16, 1)
    k, span = 0, 1
    while span < NB * steps:
        gain = gain + PK[k] * shifted(gain, span)
        k, span = k + 1, span * 2

    G[z, y, 0:1] = jnp.sum(gain, axis=0, keepdims=True)
    G[z, y, 1:2] = jnp.sum(gain * gain, axis=0, keepdims=True)
    G[z, y, 2:3] = jnp.sum(live, axis=0, keepdims=True)
    G[z, y, 3:4] = jnp.zeros((1, steps), jnp.float32)
    g_copies = []
    for k, (i, j) in enumerate(dp_peers):
        copy = remote(G.at[z, y], G.at[z, y], g_send.at[k], g_recv.at[k], {"z": wrap(z + i, NZ), "y": wrap(y + j, NY)})
        copy.start()
        g_copies.append(copy)

    back = live * (gain + v16)
    for b in range(NB):
        GN[0, b] = gain[2 * b:2 * b + 2]
        GN[1, b] = back[2 * b:2 * b + 2]
        GN[2, b] = live[2 * b:2 * b + 2]
    me = x * 2 + c
    out[1] = GN[1, me]
    for copy in v_copies + g_copies:
        copy.wait_send()
    for copy in g_copies:
        copy.wait_recv()
    sums = jnp.sum(jnp.sum(G[...], axis=(0, 1)), axis=1, keepdims=True)
    count = sums[2:3]
    mean = sums[0:1] / count
    spread = sums[1:2] / count - mean * mean
    out[0] = GN[2, me] * (GN[0, me] - mean) / jnp.sqrt(spread + 1e-06)


def on_device(sizes, hidden, first_weight, first_bias, second_weight, second_bias, rewards, dones, lengths, discount, trace):
    NZ, NY, NX = sizes
    traj, steps, feats = hidden.shape
    depth, units = first_weight.shape
    rows = traj * steps
    NB = NX * 2
    vmem = pl.BlockSpec(memory_space=pltpu.VMEM)
    hbm = pl.BlockSpec(memory_space=pltpu.HBM)
    dma = pltpu.SemaphoreType.DMA
    n_pieces = NZ * NY
    share = depth // 2 + depth // 4
    n_tm = NB - 1
    f32, bf16 = jnp.float32, jnp.bfloat16
    both = pl.pallas_call(
        functools.partial(kernel, sizes),
        out_shape=jax.ShapeDtypeStruct((2, traj, steps), f32),
        in_specs=[hbm] * 10,
        out_specs=vmem,
        scratch_shapes=[
            pltpu.VMEM((2 * rows, feats), bf16),
            pltpu.VMEM((NZ, NY, depth // 2 + share, 128), bf16),
            pltpu.VMEM((NZ, NY, depth // 2 + share, 128), bf16),
            pltpu.VMEM((NZ, NY, 2 * share, 128), bf16),
            pltpu.VMEM((2, 2 * rows, 256), f32),
            pltpu.VMEM((2, NX, 2 * traj, steps), f32),
            pltpu.VMEM((NX, 2, 4, steps), f32),
            pltpu.VMEM((10, 2 * NB, steps), f32),
            pltpu.VMEM((3, 2 * NB, steps), f32),
            pltpu.VMEM((3, NB, 2, steps), f32),
            pltpu.VMEM((NZ, NY, 4, steps), f32),
            pltpu.VMEM((traj, steps), f32),
            pltpu.VMEM((traj, steps), jnp.int32),
            pltpu.VMEM((units // 128, 128), f32),
            pltpu.VMEM((units // 128, 128), f32),
            pltpu.SMEM((traj,), jnp.int32),
            pltpu.SMEM((traj,), f32),
            pltpu.SMEM((traj,), f32),
            pltpu.SMEM((1,), f32),
            dma((15,)), dma, dma,
            dma((n_pieces,)), dma((n_pieces,)), dma((2 * n_pieces,)), dma, dma((NZ,)),
            dma((n_tm,)), dma((n_tm,)), dma((n_tm,)), dma((n_tm,)),
            dma((n_pieces - 1,)), dma((n_pieces - 1,)),
        ],
        compiler_params=pltpu.CompilerParams(collective_id=0, has_side_effects=True, vmem_limit_bytes=60 << 20),
    )(
        hidden.reshape(rows, feats), first_weight, first_bias.reshape(-1, 128), second_weight.reshape(-1, 128),
        rewards, dones, lengths, discount, trace, second_bias,
    )
    return both[0], both[1]


def solution(mesh):
    split = Mesh(mesh.devices.reshape(8, 8, 4, 2), ("z", "y", "x", "c"))
    placed = (
        P(DP, TM, None), P(DP, None), P(), P(), P(), P(DP, TM), P(DP, TM), P(DP), P(DP), P(DP),
    )
    return jax.shard_map(
        functools.partial(on_device, (8, 8, 4)),
        mesh=split, in_specs=placed, out_specs=(P(DP, TM), P(DP, TM)), check_vma=False,
    )
```

```python
import functools

import jax
import jax.numpy as jnp
from jax import lax
from jax.experimental import pallas as pl
from jax.experimental.pallas import tpu as pltpu
from jax.sharding import Mesh
from jax.sharding import PartitionSpec as P

MESH = pl.DeviceIdType.MESH
CHAIN = ((1,), (1,), (1,), (1,))
SKIP = ((1,), (1, 2), (2,), ())
SKIP2 = ((1,), (1,), (1, 2), ())
PAIRS = ((1, 2), (), (1, 2), ())
TABLES_AT = 60
ACROSS_AFTER = 24
HELD = 1
DP = ("z", "y")
TM = ("x", "c")


def offsets(n):
    return list(range(-(n // 2 - 1), n // 2 + 1))


def kernel(
    sizes,
    hid, w, b1, w2, rew, don, ln, gm, tr, b2,
    out,
    H, A, B, X, acc, T, V, RK, PK, C, GN, G, rewv, donv, b1v, w2v, lns, gms, trs, b2s,
    ld, h_send, h_recv, a_recv, b_recv, a_send, b_send, x_send, x_recv,
    rk_send, rk_recv, v_send, v_recv, g_send, g_recv,
):
    NZ, NY, NX = sizes
    NB = NX * 2
    z, y, x, c = (lax.axis_index(a) for a in ("z", "y", "x", "c"))
    (traj, steps), depth = rew.shape, w.shape[0]
    rows = traj * steps
    par = lax.rem(x, 2)
    q, e = depth // 4, depth // 2

    def wrap(v, n):
        return lax.rem(v + n, n)

    def remote(src, dst, ss, rs, dev):
        return pltpu.make_async_remote_copy(
            src_ref=src, dst_ref=dst, send_sem=ss, recv_sem=rs, device_id=dev, device_id_type=MESH
        )

    tm_peers = [(i, j) for i in range(NX) for j in range(2) if (i, j) != (0, 0)]
    dp_peers = [(i, j) for i in range(NZ) for j in range(NY) if (i, j) != (0, 0)]

    loads = []

    def load(src, dst, sem):
        copy = pltpu.make_async_copy(src, dst, ld.at[sem])
        copy.start()
        loads.append(copy)

    def block(j):
        return pl.ds(pl.multiple_of((c * 4 + j) * 128, 128), 128)

    load(rew, rewv, 2)
    load(don, donv, 3)
    own, other = 1 + 2 * par, 3 - 2 * par
    for p, W in enumerate((A, B)):
        load(w.at[p * e:(p + 1) * e, block(0)], W.at[z * NY + y, 0:e], p)
        load(w.at[p * e:(p + 1) * e, block(own)], W.at[z * NY + y, e:2 * e], p)
        load(w.at[pl.ds(pl.multiple_of(par * e + p * q, q), q), block(2)], W.at[z * NY + y, 2 * e:2 * e + q], p)
    own_h = H.at[pl.ds(pl.multiple_of(c * rows, rows), rows)]
    load(hid, own_h, 4)
    own_load = loads[-1]
    for i, (src, dst) in enumerate(((b1, b1v), (w2, w2v), (ln, lns), (gm, gms), (tr, trs), (b2, b2s))):
        load(src, dst, 5 + i)
    small_loads = loads[-6:]

    for copy in loads[:2]:
        copy.wait()
    me = x * 2 + c
    RK[me, 0:2] = rewv[...]
    RK[me, 2:4] = 1.0 - donv[...].astype(jnp.float32)

    barrier = pltpu.get_barrier_semaphore()
    near = [{"z": wrap(z + d, NZ)} for d in (1, -1, 2, -2)] + [{"y": wrap(y + d, NY)} for d in (1, -1, 2, -2)]
    far = [{"x": wrap(x + i, NX), "c": wrap(c + j, 2)} for i, j in tm_peers]
    for dev in near + far:
        pl.semaphore_signal(barrier, inc=1, device_id=dev, device_id_type=MESH)
    pl.semaphore_wait(barrier, len(near) + len(far))
    for p, W in enumerate((A, B)):
        spot = W.at[z * NY + y]
        pltpu.make_async_copy(spot, spot, ld.at[p]).wait()

    oz, oy = offsets(NZ), offsets(NY)
    sends = []
    n_oz = len(oz)
    sem_of = {(ry, rz): (ry - oy[0]) * n_oz + (rz - oz[0]) for ry in oy for rz in oz}
    zabs = {rz: wrap(z + rz, NZ) for rz in oz}
    yabs = {ry: wrap(y + ry, NY) for ry in oy}

    def place(part, piece):
        ry, rz = piece
        return (A, B)[part].at[zabs[rz] * NY + yabs[ry]]

    def norm(o, n):
        return o + n if o < -(n // 2 - 1) else o

    def hop(part, piece, axis, by):
        ry, rz = piece
        sem = (a_recv, b_recv)[part]
        there = (ry, norm(rz - by, NZ)) if axis == "z" else (norm(ry - by, NY), rz)
        here, n = (z, NZ) if axis == "z" else (y, NY)
        spot = place(part, piece)
        copy = remote(spot, spot, (a_send, b_send)[part], sem.at[sem_of[there]], {axis: wrap(here + by, n)})
        copy.start()
        sends.append(copy)

    def across(part, piece):
        ry, rz = piece
        src = place(part, piece).at[e:2 * e + q]
        dst = X.at[zabs[rz] * NY + yabs[ry], part * (e + q):(part + 1) * (e + q)]
        by = 1 - 2 * part
        remote(src, dst, x_send, x_recv.at[rz - oz[0]], {"x": wrap(x + by, NX)}).start()

    def forwards(part, piece):
        ry, rz = piece
        (ax1, n1, o1), (ax2, n2, o2) = (("z", NZ, rz), ("y", NY, ry)) if part == 0 else (("y", NY, ry), ("z", NZ, rz))
        first, second = [], []

        def onward(tree, n, o, last):
            out = []
            for way in (1, -1):
                if o == 0 or ((o < 0) == (way > 0) and abs(o) < n // 2):
                    for j in tree[abs(o)]:
                        d = abs(o) + j
                        if d < n // 2 or (d == n // 2 and way == last):
                            out.append(way * j)
            return out

        if o2 == 0:
            first = [(ax1, by) for by in onward(PAIRS, n1, o1, 1)]
        tree = SKIP if abs(o1) >= 3 else CHAIN
        second = [(ax2, by) for by in onward(tree, n2, o2, 1 if o1 % 2 == 0 else -1)]
        return first + second

    for part in (0, 1):
        for axis, by in forwards(part, (0, 0)):
            hop(part, (0, 0), axis, by)
        across(part, (0, 0))

    mate = {"c": 1 - c}
    h_copy = remote(hid, own_h, h_send, h_recv, mate)
    h_copy.start()
    for k, (i, j) in enumerate(tm_peers):
        remote(RK.at[me], RK.at[me], rk_send, rk_recv, far[k]).start()

    def arrived(ref, sem):
        spots = ref.at[0:ref.shape[0] - 1]
        pltpu.make_async_copy(spots, spots, sem).wait()

    def tables():
        arrived(RK, rk_recv)
        for copy in small_loads:
            copy.wait()
        rew16 = jnp.concatenate([RK[b, 0:2] for b in range(NB)], axis=0)
        keep16 = jnp.concatenate([RK[b, 2:4] for b in range(NB)], axis=0)
        row = lax.broadcasted_iota(jnp.int32, rew16.shape, 0)
        lane = lax.broadcasted_iota(jnp.int32, rew16.shape, 1)
        t = (row // 2) * steps + lane
        odd = row % 2 == 1
        length = jnp.where(odd, lns[1], lns[0])
        gamma = jnp.where(odd, gms[1], gms[0])
        lam = jnp.where(odd, trs[1], trs[0])
        live = (t < length).astype(jnp.float32)
        live_next = (t + 1 < length).astype(jnp.float32)
        C[0] = live
        C[1] = live * rew16
        C[2] = live * gamma * keep16 * live_next
        prod = gamma * lam * keep16 * live_next
        k, span = 0, 1
        while span < NB * steps:
            PK[k] = prod
            prod = prod * shifted(prod, span)
            k, span = k + 1, span * 2

    def shifted(v, span):
        n = NB * 2
        if span >= steps:
            r = 2 * (span // steps)
            return jnp.concatenate([v[r:], v[:r]], axis=0)
        rolled = pltpu.roll(v, steps - span, 1)
        lane = lax.broadcasted_iota(jnp.int32, v.shape, 1)
        return jnp.where(lane < steps - span, rolled, jnp.concatenate([rolled[2:], rolled[:2]], axis=0))

    def hidden_rows(rz, r):
        k = NY * depth
        return H[pl.ds(r * rows, rows), pl.ds(pl.multiple_of(zabs[rz] * k, k), k)]

    def multiply(p, rz, blocks, first):
        wv = jnp.concatenate([jnp.concatenate(b, axis=0) for b in blocks], axis=1)
        for r in range(2):
            rs = pl.ds(r * rows, rows)
            d = jnp.dot(hidden_rows(rz, r), wv, preferred_element_type=jnp.float32)
            if first:
                acc[p, rs] = d
            else:
                acc[p, rs] += d

    def own_part(rz, first):
        zz = zabs[rz]
        block0 = [W[zz * NY + j, 0:e] for j in range(NY) for W in (A, B)]
        mine = [W[zz * NY + j, e:2 * e] for j in range(NY) for W in (A, B)]
        multiply(0, rz, (block0, mine), first)

    def projected(p, r):
        rs = pl.ds(r * steps, steps)
        total = None
        for j, u in enumerate(((0, own), (other, 2))[p]):
            u = c * 4 + u
            h = 0.5 * (acc[p, rs, j * 128:(j + 1) * 128] + b1v[pl.ds(u, 1), :])
            term = (h + h * jnp.tanh(h)) * w2v[pl.ds(u, 1), :]
            total = term if total is None else total + term
        return total

    def across_part(rz, first):
        zz = zabs[rz]
        spots = X.at[pl.ds(zz * NY, NY)]
        pltpu.make_async_copy(spots, spots, x_recv.at[rz - oz[0]]).wait()
        theirs, block2 = [], []
        for j in range(NY):
            theirs += [X[zz * NY + j, 0:e], X[zz * NY + j, e + q:2 * e + q]]
            a = jnp.concatenate([A[zz * NY + j, 2 * e:], B[zz * NY + j, 2 * e:]], axis=0)
            b = jnp.concatenate([X[zz * NY + j, e:e + q], X[zz * NY + j, 2 * e + q:]], axis=0)
            block2 += [jnp.where(par == 0, a, b), jnp.where(par == 0, b, a)]
        multiply(1, rz, (theirs, block2), first)

    def passed(part, piece):
        for axis, by in forwards(part, piece):
            hop(part, piece, axis, by)
        across(part, piece)

    def delay(tree, o):
        best = {0: 0.0}
        for d in range(abs(o)):
            for j in tree[d] if d in best else ():
                best[d + j] = best[d] + 1.9 + 0.5 * j
        return best[abs(o)]

    def arrival(part, piece):
        o1, o2 = (piece[1], piece[0]) if part == 0 else piece
        return delay(PAIRS, o1) + delay(SKIP if abs(o1) >= 3 else CHAIN, o2) + 0.1 * abs(o2)

    pieces = [(p, (ry, rz)) for p in (0, 1) for ry in oy for rz in oz if (ry, rz) != (0, 0)]
    pieces.sort(key=lambda e: (arrival(*e), e[1], e[0]))
    events = [(i, 0, p, piece) for i, (p, piece) in enumerate(pieces)]
    for rz in oz:
        done = max(i for i, _, _, piece in events if type(piece) is tuple and piece[1] == rz)
        events.append((done, 1, 0, rz))
        events.append((done + ACROSS_AFTER, 2, 0, rz))
    events.append((TABLES_AT, 3, 0, 0))
    firsts = {1: True, 2: True}
    held = []
    rows_left = NZ
    for t, kind, part, what in sorted(events, key=lambda ev: ev[:2]):
        if kind == 0:
            spot = place(part, what)
            pltpu.make_async_copy(spot, spot, (a_recv, b_recv)[part].at[sem_of[what]]).wait()
            if t < HELD:
                held.append((part, what))
                if t == HELD - 1:
                    for one in held:
                        passed(*one)
            else:
                passed(part, what)
        elif kind == 3:
            tables()
        else:
            if kind == 1 and firsts[1]:
                own_load.wait()
                h_copy.wait_recv()
            (own_part if kind == 1 else across_part)(what, firsts[kind])
            firsts[kind] = False
            if kind == 1:
                rows_left -= 1
                if rows_left == 0:
                    for r in range(2 * traj):
                        T[r] = projected(0, r)

    for r in range(2 * traj):
        V[c * NX + x, r:r + 1] = jnp.sum((T[r] + projected(1, r)).T, axis=0, keepdims=True)

    for dev in far:
        remote(V.at[c * NX + x], V.at[c * NX + x], v_send, v_recv, dev).start()
    assert len(sends) == 2 * (NZ * NY - 1)
    arrived(A, a_send)
    arrived(B, b_send)
    pltpu.make_async_copy(X, X, x_send).wait()
    h_copy.wait_send()
    arrived(RK, rk_send)
    arrived(V, v_recv)

    both = V[0:NX] + V[NX:]
    v16 = jnp.concatenate([both[b // 2, 2 * (b % 2):2 * (b % 2) + 2] for b in range(NB)], axis=0) + b2s[0, 0]
    live = C[0]
    gain = C[1] - live * v16 + C[2] * shifted(v16, 1)
    k, span = 0, 1
    while span < NB * steps:
        gain = gain + PK[k] * shifted(gain, span)
        k, span = k + 1, span * 2

    G[z * NY + y, 0:1] = jnp.sum(gain, axis=0, keepdims=True)
    G[z * NY + y, 1:2] = jnp.sum(gain * gain, axis=0, keepdims=True)
    G[z * NY + y, 2:3] = jnp.sum(live, axis=0, keepdims=True)
    G[z * NY + y, 3:4] = jnp.zeros((1, steps), jnp.float32)
    for i, j in dp_peers:
        spot = G.at[z * NY + y]
        remote(spot, spot, g_send, g_recv, {"z": wrap(z + i, NZ), "y": wrap(y + j, NY)}).start()

    back = live * (gain + v16)
    for b in range(NB):
        GN[0, b] = gain[2 * b:2 * b + 2]
        GN[1, b] = back[2 * b:2 * b + 2]
        GN[2, b] = live[2 * b:2 * b + 2]
    out[1] = GN[1, me]
    arrived(V, v_send)
    arrived(G, g_send)
    arrived(G, g_recv)
    sums = jnp.sum(jnp.sum(G[...], axis=0), axis=1, keepdims=True)
    count = sums[2:3]
    mean = sums[0:1] / count
    spread = sums[1:2] / count - mean * mean
    out[0] = GN[2, me] * (GN[0, me] - mean) / jnp.sqrt(spread + 1e-06)


def on_device(sizes, hidden, first_weight, first_bias, second_weight, second_bias, rewards, dones, lengths, discount, trace):
    NZ, NY, NX = sizes
    traj, steps, feats = hidden.shape
    depth, units = first_weight.shape
    rows = traj * steps
    NB = NX * 2
    vmem = pl.BlockSpec(memory_space=pltpu.VMEM)
    hbm = pl.BlockSpec(memory_space=pltpu.HBM)
    dma = pltpu.SemaphoreType.DMA
    n_pieces = NZ * NY
    share = depth // 2 + depth // 4
    f32, bf16 = jnp.float32, jnp.bfloat16
    both = pl.pallas_call(
        functools.partial(kernel, sizes),
        out_shape=jax.ShapeDtypeStruct((2, traj, steps), f32),
        in_specs=[hbm] * 10,
        out_specs=vmem,
        scratch_shapes=[
            pltpu.VMEM((2 * rows, feats), bf16),
            pltpu.VMEM((NZ * NY, depth // 2 + share, 128), bf16),
            pltpu.VMEM((NZ * NY, depth // 2 + share, 128), bf16),
            pltpu.VMEM((NZ * NY, 2 * share, 128), bf16),
            pltpu.VMEM((2, 2 * rows, 256), f32),
            pltpu.VMEM((2 * traj, steps, 128), f32),
            pltpu.VMEM((NB, 2 * traj, steps), f32),
            pltpu.VMEM((NB, 4, steps), f32),
            pltpu.VMEM((10, 2 * NB, steps), f32),
            pltpu.VMEM((3, 2 * NB, steps), f32),
            pltpu.VMEM((3, NB, 2, steps), f32),
            pltpu.VMEM((NZ * NY, 4, steps), f32),
            pltpu.VMEM((traj, steps), f32),
            pltpu.VMEM((traj, steps), jnp.int32),
            pltpu.VMEM((units // 128, 128), f32),
            pltpu.VMEM((units // 128, 128), f32),
            pltpu.SMEM((traj,), jnp.int32),
            pltpu.SMEM((traj,), f32),
            pltpu.SMEM((traj,), f32),
            pltpu.SMEM((1, 1), f32),
            dma((11,)), dma, dma,
            dma((n_pieces,)), dma((n_pieces,)), dma, dma, dma, dma((NZ,)),
            dma, dma, dma, dma, dma, dma,
        ],
        compiler_params=pltpu.CompilerParams(collective_id=0, has_side_effects=True, vmem_limit_bytes=60 << 20),
    )(
        hidden.reshape(rows, feats), first_weight, first_bias.reshape(-1, 128), second_weight.reshape(-1, 128),
        rewards, dones, lengths, discount, trace, second_bias.reshape(1, 1),
    )
    return both[0], both[1]


def solution(mesh):
    split = Mesh(mesh.devices.reshape(8, 8, 4, 2), ("z", "y", "x", "c"))
    placed = (
        P(DP, TM, None), P(DP, None), P(), P(), P(), P(DP, TM), P(DP, TM), P(DP), P(DP), P(DP),
    )
    return jax.shard_map(
        functools.partial(on_device, (8, 8, 4)),
        mesh=split, in_specs=placed, out_specs=(P(DP, TM), P(DP, TM)), check_vma=False,
    )
```

```python
import functools

import jax
import jax.numpy as jnp
from jax import lax
from jax.experimental import pallas as pl
from jax.experimental.pallas import tpu as pltpu
from jax.sharding import Mesh
from jax.sharding import PartitionSpec as P

MESH = pl.DeviceIdType.MESH
CHAIN = ((1,), (1,), (1,), (1,))
SKIP = ((1,), (1, 2), (2,), ())
SKIP2 = ((1,), (1,), (1, 2), ())
PAIRS = ((1, 2), (), (1, 2), ())
TABLES_AT = 11.5
ACROSS_AFTER = 24
HELD = 1
DP = ("z", "y")
TM = ("x", "c")


def offsets(n):
    return list(range(-(n // 2 - 1), n // 2 + 1))


def kernel(
    sizes,
    hid, w, b1, w2, rew, don, ln, gm, tr, b2,
    out,
    H, A, B, X, acc, T, V, RK, PK, C, GN, G, rewv, donv, b1v, w2v, lns, gms, trs, b2s,
    ld, h_send, h_recv, a_recv, b_recv, a_send, b_send, x_send, x_recv,
    rk_send, rk_recv, v_send, v_recv, g_send, g_recv,
):
    NZ, NY, NX = sizes
    NB = NX * 2
    z, y, x, c = (lax.axis_index(a) for a in ("z", "y", "x", "c"))
    (traj, steps), depth = rew.shape, w.shape[0]
    rows = traj * steps
    par = lax.rem(x, 2)
    q, e = depth // 4, depth // 2

    def wrap(v, n):
        return lax.rem(v + n, n)

    def remote(src, dst, ss, rs, dev):
        return pltpu.make_async_remote_copy(
            src_ref=src, dst_ref=dst, send_sem=ss, recv_sem=rs, device_id=dev, device_id_type=MESH
        )

    tm_peers = [(i, j) for i in range(NX) for j in range(2) if (i, j) != (0, 0)]
    dp_peers = [(i, j) for i in range(NZ) for j in range(NY) if (i, j) != (0, 0)]

    loads = []

    def load(src, dst, sem):
        copy = pltpu.make_async_copy(src, dst, ld.at[sem])
        copy.start()
        loads.append(copy)

    def block(j):
        return pl.ds(pl.multiple_of((c * 4 + j) * 128, 128), 128)

    load(rew, rewv, 2)
    load(don, donv, 3)
    own, other = 1 + 2 * par, 3 - 2 * par
    for p, W in enumerate((A, B)):
        load(w.at[p * e:(p + 1) * e, block(0)], W.at[z * NY + y, 0:e], p)
        load(w.at[p * e:(p + 1) * e, block(own)], W.at[z * NY + y, e:2 * e], p)
        load(w.at[pl.ds(pl.multiple_of(par * e + p * q, q), q), block(2)], W.at[z * NY + y, 2 * e:2 * e + q], p)
    own_h = H.at[pl.ds(pl.multiple_of(c * rows, rows), rows)]
    load(hid, own_h, 4)
    own_load = loads[-1]
    for i, (src, dst) in enumerate(((b1, b1v), (w2, w2v), (ln, lns), (gm, gms), (tr, trs), (b2, b2s))):
        load(src, dst, 5 + i)
    small_loads = loads[-6:]

    for copy in loads[:2]:
        copy.wait()
    me = x * 2 + c
    RK[me, 0:2] = rewv[...]
    RK[me, 2:4] = 1.0 - donv[...].astype(jnp.float32)

    barrier = pltpu.get_barrier_semaphore()
    near = [{"z": wrap(z + d, NZ)} for d in (1, -1, 2, -2)] + [{"y": wrap(y + d, NY)} for d in (1, -1, 2, -2)]
    far = [{"x": wrap(x + i, NX), "c": wrap(c + j, 2)} for i, j in tm_peers]
    for dev in near + far:
        pl.semaphore_signal(barrier, inc=1, device_id=dev, device_id_type=MESH)
    pl.semaphore_wait(barrier, len(near) + len(far))
    for p, W in enumerate((A, B)):
        spot = W.at[z * NY + y]
        pltpu.make_async_copy(spot, spot, ld.at[p]).wait()

    oz, oy = offsets(NZ), offsets(NY)
    sends = []
    n_oz = len(oz)
    sem_of = {(ry, rz): (ry - oy[0]) * n_oz + (rz - oz[0]) for ry in oy for rz in oz}
    zabs = {rz: wrap(z + rz, NZ) for rz in oz}
    yabs = {ry: wrap(y + ry, NY) for ry in oy}

    def place(part, piece):
        ry, rz = piece
        return (A, B)[part].at[zabs[rz] * NY + yabs[ry]]

    def norm(o, n):
        return o + n if o < -(n // 2 - 1) else o

    def hop(part, piece, axis, by):
        ry, rz = piece
        sem = (a_recv, b_recv)[part]
        there = (ry, norm(rz - by, NZ)) if axis == "z" else (norm(ry - by, NY), rz)
        here, n = (z, NZ) if axis == "z" else (y, NY)
        spot = place(part, piece)
        copy = remote(spot, spot, (a_send, b_send)[part], sem.at[sem_of[there]], {axis: wrap(here + by, n)})
        copy.start()
        sends.append(copy)

    def across(part, piece):
        ry, rz = piece
        src = place(part, piece).at[e:2 * e + q]
        dst = X.at[zabs[rz] * NY + yabs[ry], part * (e + q):(part + 1) * (e + q)]
        by = 1 - 2 * part
        remote(src, dst, x_send, x_recv.at[rz - oz[0]], {"x": wrap(x + by, NX)}).start()

    def forwards(part, piece):
        ry, rz = piece
        (ax1, n1, o1), (ax2, n2, o2) = (("z", NZ, rz), ("y", NY, ry)) if part == 0 else (("y", NY, ry), ("z", NZ, rz))
        first, second = [], []

        def onward(tree, n, o, last):
            out = []
            for way in (1, -1):
                if o == 0 or ((o < 0) == (way > 0) and abs(o) < n // 2):
                    for j in tree[abs(o)]:
                        d = abs(o) + j
                        if d < n // 2 or (d == n // 2 and way == last):
                            out.append(way * j)
            return out

        if o2 == 0:
            first = [(ax1, by) for by in onward(PAIRS, n1, o1, 1)]
        tree = SKIP if abs(o1) >= 4 else CHAIN
        second = [(ax2, by) for by in onward(tree, n2, o2, 1 if o1 % 2 == 0 else -1)]
        return first + second

    for part in (0, 1):
        for axis, by in forwards(part, (0, 0)):
            hop(part, (0, 0), axis, by)
        across(part, (0, 0))

    mate = {"c": 1 - c}
    h_copy = remote(hid, own_h, h_send, h_recv, mate)
    h_copy.start()
    for k, (i, j) in enumerate(tm_peers):
        remote(RK.at[me], RK.at[me], rk_send, rk_recv, far[k]).start()

    def arrived(ref, sem):
        spots = ref.at[0:ref.shape[0] - 1]
        pltpu.make_async_copy(spots, spots, sem).wait()

    def tables():
        arrived(RK, rk_recv)
        for copy in small_loads:
            copy.wait()
        rew16 = jnp.concatenate([RK[b, 0:2] for b in range(NB)], axis=0)
        keep16 = jnp.concatenate([RK[b, 2:4] for b in range(NB)], axis=0)
        row = lax.broadcasted_iota(jnp.int32, rew16.shape, 0)
        lane = lax.broadcasted_iota(jnp.int32, rew16.shape, 1)
        t = (row // 2) * steps + lane
        odd = row % 2 == 1
        length = jnp.where(odd, lns[1], lns[0])
        gamma = jnp.where(odd, gms[1], gms[0])
        lam = jnp.where(odd, trs[1], trs[0])
        live = (t < length).astype(jnp.float32)
        live_next = (t + 1 < length).astype(jnp.float32)
        C[0] = live
        C[1] = live * rew16
        C[2] = live * gamma * keep16 * live_next
        prod = gamma * lam * keep16 * live_next
        k, span = 0, 1
        while span < NB * steps:
            PK[k] = prod
            prod = prod * shifted(prod, span)
            k, span = k + 1, span * 2

    def shifted(v, span):
        n = NB * 2
        if span >= steps:
            r = 2 * (span // steps)
            return jnp.concatenate([v[r:], v[:r]], axis=0)
        rolled = pltpu.roll(v, steps - span, 1)
        lane = lax.broadcasted_iota(jnp.int32, v.shape, 1)
        return jnp.where(lane < steps - span, rolled, jnp.concatenate([rolled[2:], rolled[:2]], axis=0))

    def hidden_rows(rz, r):
        k = NY * depth
        return H[pl.ds(r * rows, rows), pl.ds(pl.multiple_of(zabs[rz] * k, k), k)]

    def multiply(p, rz, blocks, first):
        wv = jnp.concatenate([jnp.concatenate(b, axis=0) for b in blocks], axis=1)
        for r in range(2):
            rs = pl.ds(r * rows, rows)
            d = jnp.dot(hidden_rows(rz, r), wv, preferred_element_type=jnp.float32)
            if first:
                acc[p, rs] = d
            else:
                acc[p, rs] += d

    def own_part(rz, first):
        zz = zabs[rz]
        block0 = [W[zz * NY + j, 0:e] for j in range(NY) for W in (A, B)]
        mine = [W[zz * NY + j, e:2 * e] for j in range(NY) for W in (A, B)]
        multiply(0, rz, (block0, mine), first)

    def projected(p, r):
        rs = pl.ds(r * steps, steps)
        total = None
        for j, u in enumerate(((0, own), (other, 2))[p]):
            u = c * 4 + u
            h = 0.5 * (acc[p, rs, j * 128:(j + 1) * 128] + b1v[pl.ds(u, 1), :])
            term = (h + h * jnp.tanh(h)) * w2v[pl.ds(u, 1), :]
            total = term if total is None else total + term
        return total

    def across_part(rz, first):
        zz = zabs[rz]
        spots = X.at[pl.ds(zz * NY, NY)]
        pltpu.make_async_copy(spots, spots, x_recv.at[rz - oz[0]]).wait()
        theirs, block2 = [], []
        for j in range(NY):
            theirs += [X[zz * NY + j, 0:e], X[zz * NY + j, e + q:2 * e + q]]
            a = jnp.concatenate([A[zz * NY + j, 2 * e:], B[zz * NY + j, 2 * e:]], axis=0)
            b = jnp.concatenate([X[zz * NY + j, e:e + q], X[zz * NY + j, 2 * e + q:]], axis=0)
            block2 += [jnp.where(par == 0, a, b), jnp.where(par == 0, b, a)]
        multiply(1, rz, (theirs, block2), first)

    def passed(part, piece):
        for axis, by in forwards(part, piece):
            hop(part, piece, axis, by)
        across(part, piece)

    def delay(tree, o):
        best = {0: 0.0}
        for d in range(abs(o)):
            for j in tree[d] if d in best else ():
                best[d + j] = best[d] + 1.9 + 0.5 * j
        return best[abs(o)]

    def arrival(part, piece):
        o1, o2 = (piece[1], piece[0]) if part == 0 else piece
        return delay(PAIRS, o1) + delay(SKIP if abs(o1) >= 4 else CHAIN, o2) + 0.6 * abs(o2)

    pieces = [(p, (ry, rz)) for p in (0, 1) for ry in oy for rz in oz if (ry, rz) != (0, 0)]
    pieces.sort(key=lambda e: (arrival(*e), e[1], e[0]))
    events = [(i, 0, p, piece) for i, (p, piece) in enumerate(pieces)]
    for rz in oz:
        done = max(i for i, _, _, piece in events if type(piece) is tuple and piece[1] == rz)
        events.append((done, 1, 0, rz))
        events.append((done + ACROSS_AFTER, 2, 0, rz))
    events.append((TABLES_AT, 3, 0, 0))
    firsts = {1: True, 2: True}
    held = []
    rows_left = NZ
    for t, kind, part, what in sorted(events, key=lambda ev: ev[:2]):
        if kind == 0:
            spot = place(part, what)
            pltpu.make_async_copy(spot, spot, (a_recv, b_recv)[part].at[sem_of[what]]).wait()
            if t < HELD:
                held.append((part, what))
                if t == HELD - 1:
                    for one in held:
                        passed(*one)
            else:
                passed(part, what)
        elif kind == 3:
            tables()
        else:
            if kind == 1 and firsts[1]:
                own_load.wait()
                h_copy.wait_recv()
            (own_part if kind == 1 else across_part)(what, firsts[kind])
            firsts[kind] = False
            if kind == 1:
                rows_left -= 1
                if rows_left == 0:
                    for r in range(2 * traj):
                        T[r] = projected(0, r)

    for r in range(2 * traj):
        V[c * NX + x, r:r + 1] = jnp.sum((T[r] + projected(1, r)).T, axis=0, keepdims=True)

    for dev in far:
        remote(V.at[c * NX + x], V.at[c * NX + x], v_send, v_recv, dev).start()
    assert len(sends) == 2 * (NZ * NY - 1)
    arrived(A, a_send)
    arrived(B, b_send)
    pltpu.make_async_copy(X, X, x_send).wait()
    h_copy.wait_send()
    arrived(RK, rk_send)
    arrived(V, v_recv)

    both = V[0:NX] + V[NX:]
    v16 = jnp.concatenate([both[b // 2, 2 * (b % 2):2 * (b % 2) + 2] for b in range(NB)], axis=0) + b2s[0, 0]
    live = C[0]
    gain = C[1] - live * v16 + C[2] * shifted(v16, 1)
    k, span = 0, 1
    while span < NB * steps:
        gain = gain + PK[k] * shifted(gain, span)
        k, span = k + 1, span * 2

    G[z * NY + y, 0:1] = jnp.sum(gain, axis=0, keepdims=True)
    G[z * NY + y, 1:2] = jnp.sum(gain * gain, axis=0, keepdims=True)
    G[z * NY + y, 2:3] = jnp.sum(live, axis=0, keepdims=True)
    G[z * NY + y, 3:4] = jnp.zeros((1, steps), jnp.float32)
    for i, j in dp_peers:
        spot = G.at[z * NY + y]
        remote(spot, spot, g_send, g_recv, {"z": wrap(z + i, NZ), "y": wrap(y + j, NY)}).start()

    back = live * (gain + v16)
    for b in range(NB):
        GN[0, b] = gain[2 * b:2 * b + 2]
        GN[1, b] = back[2 * b:2 * b + 2]
        GN[2, b] = live[2 * b:2 * b + 2]
    out[1] = GN[1, me]
    arrived(V, v_send)
    arrived(G, g_send)
    arrived(G, g_recv)
    sums = jnp.sum(jnp.sum(G[...], axis=0), axis=1, keepdims=True)
    count = sums[2:3]
    mean = sums[0:1] / count
    spread = sums[1:2] / count - mean * mean
    out[0] = GN[2, me] * (GN[0, me] - mean) / jnp.sqrt(spread + 1e-06)


def on_device(sizes, hidden, first_weight, first_bias, second_weight, second_bias, rewards, dones, lengths, discount, trace):
    NZ, NY, NX = sizes
    traj, steps, feats = hidden.shape
    depth, units = first_weight.shape
    rows = traj * steps
    NB = NX * 2
    vmem = pl.BlockSpec(memory_space=pltpu.VMEM)
    hbm = pl.BlockSpec(memory_space=pltpu.HBM)
    dma = pltpu.SemaphoreType.DMA
    n_pieces = NZ * NY
    share = depth // 2 + depth // 4
    f32, bf16 = jnp.float32, jnp.bfloat16
    both = pl.pallas_call(
        functools.partial(kernel, sizes),
        out_shape=jax.ShapeDtypeStruct((2, traj, steps), f32),
        in_specs=[hbm] * 10,
        out_specs=vmem,
        scratch_shapes=[
            pltpu.VMEM((2 * rows, feats), bf16),
            pltpu.VMEM((NZ * NY, depth // 2 + share, 128), bf16),
            pltpu.VMEM((NZ * NY, depth // 2 + share, 128), bf16),
            pltpu.VMEM((NZ * NY, 2 * share, 128), bf16),
            pltpu.VMEM((2, 2 * rows, 256), f32),
            pltpu.VMEM((2 * traj, steps, 128), f32),
            pltpu.VMEM((NB, 2 * traj, steps), f32),
            pltpu.VMEM((NB, 4, steps), f32),
            pltpu.VMEM((10, 2 * NB, steps), f32),
            pltpu.VMEM((3, 2 * NB, steps), f32),
            pltpu.VMEM((3, NB, 2, steps), f32),
            pltpu.VMEM((NZ * NY, 4, steps), f32),
            pltpu.VMEM((traj, steps), f32),
            pltpu.VMEM((traj, steps), jnp.int32),
            pltpu.VMEM((units // 128, 128), f32),
            pltpu.VMEM((units // 128, 128), f32),
            pltpu.SMEM((traj,), jnp.int32),
            pltpu.SMEM((traj,), f32),
            pltpu.SMEM((traj,), f32),
            pltpu.SMEM((1, 1), f32),
            dma((11,)), dma, dma,
            dma((n_pieces,)), dma((n_pieces,)), dma, dma, dma, dma((NZ,)),
            dma, dma, dma, dma, dma, dma,
        ],
        compiler_params=pltpu.CompilerParams(collective_id=0, has_side_effects=True, vmem_limit_bytes=60 << 20),
    )(
        hidden.reshape(rows, feats), first_weight, first_bias.reshape(-1, 128), second_weight.reshape(-1, 128),
        rewards, dones, lengths, discount, trace, second_bias.reshape(1, 1),
    )
    return both[0], both[1]


def solution(mesh):
    split = Mesh(mesh.devices.reshape(8, 8, 4, 2), ("z", "y", "x", "c"))
    placed = (
        P(DP, TM, None), P(DP, None), P(), P(), P(), P(DP, TM), P(DP, TM), P(DP), P(DP), P(DP),
    )
    return jax.shard_map(
        functools.partial(on_device, (8, 8, 4)),
        mesh=split, in_specs=placed, out_specs=(P(DP, TM), P(DP, TM)), check_vma=False,
    )
```
